32 devices in a mesh: dp: 2 (over core), seq: 8 (over z, x), mp: 2 (over y).
Axes of the slice: x: 2, y: 2, z: 4, core: 2. Of those that a mesh axis runs over, the one named last changes fastest.
Arguments:
- queries: bfloat16 [4, 1024, 4096], P('dp', 'seq', 'mp'), may hold values from -6 to 6
- vision: bfloat16 [4, 640, 4096], P('dp', 'seq'), may hold values from -6 to 6
- key_weight: bfloat16 [4096, 1024], P(None, 'mp'), may hold values from -0.09375 to 0.09375
- value_weight: bfloat16 [4096, 1024], P(None, 'mp'), may hold values from -0.09375 to 0.09375
- query_gain: float32 [128], replicated, may hold values from 0.6 to 6
- key_gain: float32 [128], replicated, may hold values from 0.6 to 6
- out_grad: bfloat16 [4, 1024, 4096], P('dp', 'seq', 'mp'), may hold values from -6 to 6
- tile_count: int32 [4], P('dp'), may hold values from 1 to 4, as said below
Outputs:
- query_grad: bfloat16 [4, 1024, 4096], P('dp', 'seq', 'mp')
- vision_grad: bfloat16 [4, 640, 4096], P('dp', 'seq', 'mp')
- key_weight_grad: float32 [4096, 1024], P(None, 'mp')
- value_weight_grad: float32 [4096, 1024], P(None, 'mp')
The draws below stay inside these ranges and needn't reach their ends.
Inputs may be any that keep to these rules, and one draw needn't show every extreme that they name: The live vision tokens of sample s are its first tile_count[s] * 160; some sample has 4 tiles and some other sample has 1.
All inputs are finite; a program needn't handle non-finite values.
Results may differ from the reference program's by a relative error of at most 0.03.
The reference program's roundings to bfloat16 on the way (of `keys`, `values`, `normed`, `probs_b`, `attn`, `dscores`, `key_grad` and `value_grad`) count: a program that leaves them out, or rounds other values in their place, can miss the bound.
Values may be sent and summed in bfloat16 or wider, within the bound.
A program may use at most 128 MiB of HBM per device.

```python
import jax
import jax.numpy as jnp
from jax import lax

D = 4096
HEADS = 32
KV_HEADS = 8
HEAD_DIM = 128
MAX_TILES = 4
SAMPLES = 4
TXT = 1024
VIS = 640
TILE_TOK = 160


def vision_field(key):
    drawn = jax.random.normal(jax.random.fold_in(key, 7001), (SAMPLES, VIS, D), jnp.float32)
    return jnp.clip(drawn, -6.0, 6.0)


def key_matrix(key):
    drawn = jax.random.normal(jax.random.fold_in(key, 7002), (D, KV_HEADS * HEAD_DIM), jnp.float32)
    return jnp.clip(drawn, -6.0, 6.0) * D ** (-0.5)


def draw_vision(key, part):
    return vision_field(key).astype(jnp.bfloat16)


def draw_key_weight(key, part):
    return key_matrix(key).astype(jnp.bfloat16)


def draw_queries(key, part):
    drawn = jax.random.normal(jax.random.fold_in(key, 7003), (SAMPLES, TXT, HEADS * HEAD_DIM), jnp.float32)
    drawn = jnp.clip(drawn, -6.0, 6.0)
    return drawn.astype(jnp.bfloat16)


def draw_query_gain(key, part):
    inner = jax.random.fold_in(key, 7005)
    return jax.random.uniform(inner, (HEAD_DIM,), jnp.float32, 0.6, 1.4)


def draw_key_gain(key, part):
    inner = jax.random.fold_in(key, 7006)
    return jax.random.uniform(inner, (HEAD_DIM,), jnp.float32, 0.6, 1.4)


def draw_tile_count(key, part):
    counts = jax.random.randint(jax.random.fold_in(key, 7101), (SAMPLES,), 1, MAX_TILES + 1, dtype=jnp.int32)
    full_at = jax.random.randint(jax.random.fold_in(key, 7102), (), 0, SAMPLES, dtype=jnp.int32)
    step_to = jax.random.randint(jax.random.fold_in(key, 7103), (), 1, SAMPLES, dtype=jnp.int32)
    single_at = (full_at + step_to) % SAMPLES
    counts = counts.at[full_at].set(MAX_TILES)
    counts = counts.at[single_at].set(1)
    return counts.astype(jnp.int32)


def steps_of(stream_key, extent, pieces, smallest, top_value):
    def one(dim, shards_of):
        heights = jax.random.uniform(jax.random.fold_in(jax.random.fold_in(stream_key, 6), dim), (shards_of,), jnp.float32, smallest / len(pieces), top_value / len(pieces))
        return jnp.repeat(jnp.exp(heights), extent[dim] // shards_of).reshape((-1,) + (1,) * (len(extent) - dim - 1))

    level = one(*pieces[0])
    for cut in pieces[1:]:
        level = level * one(*cut)
    return level


def noise(own_key, dims, scale, bound, split=(), kind=jnp.bfloat16):
    values = jax.random.normal(own_key, dims, jnp.float32) * scale
    if len(split) > 0:
        values = steps_of(own_key, dims, split, -0.22, 0.18) * values
    return jnp.clip(values, min=-bound, max=bound).astype(kind)


def setup_inputs(seed: int = 0) -> dict:
    key_of = jax.random.split(jax.random.key(seed), 9)
    queries = draw_queries(jax.random.fold_in(key_of[8], 71), 0)
    vision = draw_vision(jax.random.fold_in(key_of[8], 71), 0)
    key_weight = draw_key_weight(jax.random.fold_in(key_of[8], 71), 0)
    value_weight = noise(key_of[3], (D, KV_HEADS * HEAD_DIM), D ** -0.5, 0.09375, ((1, 2),))
    query_gain = draw_query_gain(jax.random.fold_in(key_of[8], 71), 0)
    key_gain = draw_key_gain(jax.random.fold_in(key_of[8], 71), 0)
    out_grad = noise(key_of[6], (SAMPLES, TXT, HEADS * HEAD_DIM), 1.0, 6.0, ((0, 2), (1, 8), (2, 2)))
    tile_count = draw_tile_count(jax.random.fold_in(key_of[8], 71), 0)
    return {"queries": queries, "vision": vision, "key_weight": key_weight, "value_weight": value_weight, "query_gain": query_gain, "key_gain": key_gain, "out_grad": out_grad, "tile_count": tile_count}


EPS = 1e-05
NEG = -1e+30

def norm_apply(raw, gain):
    inverse = lax.rsqrt(lax.optimization_barrier(jnp.mean(raw * raw, axis=-1, keepdims=True)) + EPS)
    return (raw * inverse * gain, inverse)

def norm_back(raw, inverse, gain, upstream):
    weighted = upstream * gain
    return inverse * weighted - raw * inverse * inverse * inverse * lax.optimization_barrier(jnp.mean(weighted * raw, axis=-1, keepdims=True))

def sample_grads(queries_one, vision_one, out_one, tiles_one, key_weight, value_weight, query_gain, key_gain):
    group_size = HEADS // KV_HEADS
    score_scale = HEAD_DIM ** (-0.5)
    key_cols = key_weight.reshape(D, KV_HEADS, HEAD_DIM).transpose(1, 0, 2)
    value_cols = value_weight.reshape(D, KV_HEADS, HEAD_DIM).transpose(1, 0, 2)
    query_heads = queries_one.reshape(TXT, KV_HEADS, group_size, HEAD_DIM).transpose(1, 0, 2, 3)
    out_heads = out_one.reshape(TXT, KV_HEADS, group_size, HEAD_DIM).transpose(1, 0, 2, 3)
    live_keys = jnp.arange(VIS, dtype=jnp.int32) < tiles_one * TILE_TOK

    def one_group(vision_total, inputs):
        key_col, value_col, query_group, out_group = inputs
        key_raw = jnp.dot(vision_one, key_col, preferred_element_type=jnp.float32)
        key_normed, key_inverse = norm_apply(key_raw, key_gain)
        keys = key_normed.astype(jnp.bfloat16)
        values = jnp.dot(vision_one, value_col, preferred_element_type=jnp.float32).astype(jnp.bfloat16)
        query_raw = query_group.astype(jnp.float32)
        query_normed, query_inverse = norm_apply(query_raw, query_gain)
        normed = query_normed.astype(jnp.bfloat16)
        normed_wide = normed.astype(jnp.float32)
        keys_wide = keys.astype(jnp.float32)
        values_wide = values.astype(jnp.float32)
        out_wide = out_group.astype(jnp.float32)
        scores = jnp.einsum('tgd,jd->gtj', normed_wide, keys_wide) * score_scale
        scores = jnp.where(live_keys[None, None, :], scores, NEG)
        row_top = lax.optimization_barrier(jnp.max(scores, axis=-1, keepdims=True))
        expo = jnp.exp(scores - row_top)
        probs = expo / lax.optimization_barrier(jnp.sum(expo, axis=-1, keepdims=True))
        probs_b = probs.astype(jnp.bfloat16)
        probs_wide = probs_b.astype(jnp.float32)
        attn = jnp.einsum('gtj,jd->tgd', probs_wide, values_wide).astype(jnp.bfloat16)
        delta = lax.optimization_barrier(jnp.sum(out_wide * attn.astype(jnp.float32), axis=-1))
        dprobs = jnp.einsum('tgd,jd->gtj', out_wide, values_wide)
        dscores = (probs * (dprobs - delta.T[:, :, None])).astype(jnp.bfloat16)
        dscores_wide = dscores.astype(jnp.float32)
        dnormed = jnp.einsum('gtj,jd->tgd', dscores_wide, keys_wide) * score_scale
        dkeys = jnp.einsum('gtj,tgd->jd', dscores_wide, normed_wide) * score_scale
        dvalues = jnp.einsum('gtj,tgd->jd', probs_wide, out_wide)
        query_part = norm_back(query_raw, query_inverse, query_gain, dnormed).astype(jnp.bfloat16)
        key_grad = norm_back(key_raw, key_inverse, key_gain, dkeys).astype(jnp.bfloat16)
        value_grad = dvalues.astype(jnp.bfloat16)
        key_weight_part = jnp.dot(vision_one.T, key_grad, preferred_element_type=jnp.float32)
        value_weight_part = jnp.dot(vision_one.T, value_grad, preferred_element_type=jnp.float32)
        vision_term = jnp.dot(key_grad, key_col.T, preferred_element_type=jnp.float32)
        vision_term = vision_term + jnp.dot(value_grad, value_col.T, preferred_element_type=jnp.float32)
        return (vision_total + vision_term, (query_part, key_weight_part, value_weight_part))
    start_total = jnp.zeros((VIS, D), jnp.float32)
    vision_total, stacked = lax.scan(one_group, start_total, (key_cols, value_cols, query_heads, out_heads))
    query_parts, key_parts, value_parts = stacked
    query_grad = query_parts.transpose(1, 0, 2, 3).reshape(TXT, HEADS * HEAD_DIM)
    key_weight_part = key_parts.transpose(1, 0, 2).reshape(D, KV_HEADS * HEAD_DIM)
    value_weight_part = value_parts.transpose(1, 0, 2).reshape(D, KV_HEADS * HEAD_DIM)
    return (query_grad, vision_total.astype(jnp.bfloat16), key_weight_part, value_weight_part)

def reference(queries, vision, key_weight, value_weight, query_gain, key_gain, out_grad, tile_count):
    query_list = []
    vision_list = []
    key_weight_grad = jnp.zeros((D, KV_HEADS * HEAD_DIM), jnp.float32)
    value_weight_grad = jnp.zeros((D, KV_HEADS * HEAD_DIM), jnp.float32)
    for sample_at in range(SAMPLES):
        query_part, vision_part, key_part, value_part = sample_grads(queries[sample_at], vision[sample_at], out_grad[sample_at], tile_count[sample_at], key_weight, value_weight, query_gain, key_gain)
        query_list.append(query_part)
        vision_list.append(vision_part)
        key_weight_grad = key_weight_grad + key_part
        value_weight_grad = value_weight_grad + value_part
    return (jnp.stack(query_list), jnp.stack(vision_list), key_weight_grad, value_weight_grad)
```

```python
import functools

import jax
import jax.numpy as jnp
from jax import lax
from jax.experimental import pallas as pl
from jax.experimental.pallas import tpu as pltpu
from jax.sharding import PartitionSpec as P

MAX_TILES = 4
EPS = 1e-05
NEG = -1e30
MESH = pl.DeviceIdType.MESH
VMEM = pltpu.VMEM
F32 = jnp.float32
BF16 = jnp.bfloat16
CHUNKS = 2


def norm_back(raw, inverse, gain, upstream):
    weighted = upstream * gain
    return inverse * weighted - raw * inverse * inverse * inverse * jnp.mean(
        weighted * raw, axis=-1, keepdims=True
    )


def inverse_of(raw):
    return lax.rsqrt(jnp.mean(raw * raw, axis=-1, keepdims=True) + EPS)


def seq_of(place, n):
    half = place // (n // 2)
    along = place + half * (n - 1 - 2 * place)
    return 2 * along + half


def place_of(index, n):
    side = index % 2
    along = index // 2
    return along + side * (n - 1 - 2 * along)


def ring(n):
    here = lax.axis_index("seq")
    place = place_of(here, n)
    nexts = (seq_of((place + 1) % n, n), seq_of((place + n - 1) % n, n))
    return here, place, nexts


def greet(devices):
    barrier = pltpu.get_barrier_semaphore()
    for device in devices:
        pl.semaphore_signal(barrier, inc=1, device_id=device, device_id_type=MESH)
    pl.semaphore_wait(barrier, len(devices))


def gather_kernel(n, pairs, *refs):
    sources, outs = refs[0:2], refs[2:4]
    send_sem, recv_sem, pair_send, pair_recv = refs[4:8]
    here, place, nexts = ring(n)
    mine = lax.axis_index("dp")
    chunks = sources[0].shape[0]
    others = [(mine + shift) % pairs for shift in range(1, pairs)]
    greet([{"seq": nexts[0]}, {"seq": nexts[1]}] + [{"dp": other} for other in others])
    ring_copies, pair_copies = [], []
    for step in range(n):
        for chunk in range(chunks):
            for way in range(2):
                origin = seq_of((place + n - step) % n if way == 0 else (place + step) % n, n)
                target = outs[way].at[mine if pairs > 1 else 0, chunk, origin]
                if step == 0:
                    block = sources[way].at[chunk]
                else:
                    ring_copies[((step - 1) * chunks + chunk) * 2 + way].wait_recv()
                    block = target
                if step < n - 1:
                    copy = pltpu.make_async_remote_copy(
                        src_ref=block,
                        dst_ref=target,
                        send_sem=send_sem.at[way, step, chunk],
                        recv_sem=recv_sem.at[way, step, chunk],
                        device_id={"seq": nexts[way]},
                        device_id_type=MESH,
                    )
                    copy.start()
                    ring_copies.append(copy)
                for at, other in enumerate(others):
                    copy = pltpu.make_async_remote_copy(
                        src_ref=block,
                        dst_ref=target,
                        send_sem=pair_send.at[way, step, chunk, at],
                        recv_sem=pair_recv.at[way, step, chunk, at],
                        device_id={"dp": other},
                        device_id_type=MESH,
                    )
                    copy.start()
                    pair_copies.append(copy)
        if step == 0:
            for way in range(2):
                for chunk in range(chunks):
                    outs[way][mine if pairs > 1 else 0, chunk, here] = sources[way][chunk]
    for copy in ring_copies:
        copy.wait_send()
    for copy in pair_copies:
        copy.wait_send()
        copy.wait_recv()


def ring_gather(first, second, n, pairs, number):
    chunks, rows, columns = first.shape
    out = jax.ShapeDtypeStruct((pairs, chunks, n, rows, columns), first.dtype)
    sent = 2 * chunks * (n - 1) * rows * columns * 2
    return pl.pallas_call(
        functools.partial(gather_kernel, n, pairs),
        out_shape=(out, out),
        in_specs=[pl.BlockSpec(memory_space=VMEM)] * 2,
        out_specs=(pl.BlockSpec(memory_space=VMEM),) * 2,
        scratch_shapes=[
            pltpu.SemaphoreType.DMA((2, n, chunks)),
            pltpu.SemaphoreType.DMA((2, n, chunks)),
            pltpu.SemaphoreType.DMA((2, n, chunks, max(pairs - 1, 1))),
            pltpu.SemaphoreType.DMA((2, n, chunks, max(pairs - 1, 1))),
        ],
        compiler_params=pltpu.CompilerParams(collective_id=number, has_side_effects=True),
        cost_estimate=pl.CostEstimate(flops=100_000_000_000 // 4, bytes_accessed=sent, transcendentals=0),
        name=f"ring_gather_{number}",
    )(first, second)


def scatter_kernel(n, head_dim, key_ref, value_ref, raw_ref, gain_ref, key_out, value_out, *scratch):
    held, send_sem, recv_sem = scratch
    parts = (key_ref, value_ref)
    here, place, nexts = ring(n)
    chunks = key_ref.shape[0]
    greet([{"seq": nexts[0]}, {"seq": nexts[1]}])

    def copy_of(way, step, chunk, block):
        return pltpu.make_async_remote_copy(
            src_ref=block,
            dst_ref=held.at[way, step, chunk],
            send_sem=send_sem.at[way, step, chunk],
            recv_sem=recv_sem.at[way, step, chunk],
            device_id={"seq": nexts[way]},
            device_id_type=MESH,
        )

    def dest_of(way, step):
        if way == 0:
            return seq_of((place + 2 * n - 1 - step) % n, n)
        return seq_of((place + 1 + step) % n, n)

    copies = {}
    for chunk in range(chunks):
        for way in range(2):
            copy = copy_of(way, 0, chunk, parts[way].at[chunk, dest_of(way, 0)])
            copy.start()
            copies[way, 0, chunk] = copy
    for step in range(1, n):
        for chunk in range(chunks):
            for way in range(2):
                copies[way, step - 1, chunk].wait_recv()
                own = parts[way][chunk, dest_of(way, step)].astype(F32)
                total = held[way, step - 1, chunk].astype(F32) + own
                if step < n - 1:
                    held[way, step - 1, chunk] = total.astype(BF16)
                elif way == 1:
                    value_out[chunk] = total.astype(BF16)
                else:
                    gain = gain_ref[...]
                    for at in range(total.shape[1] // head_dim):
                        cut = slice(at * head_dim, (at + 1) * head_dim)
                        raw = raw_ref[chunk, :, cut]
                        grad = norm_back(raw, inverse_of(raw), gain, total[:, cut])
                        key_out[chunk, :, cut] = grad.astype(BF16)
            if step < n - 1:
                for way in range(2):
                    copy = copy_of(way, step, chunk, held.at[way, step - 1, chunk])
                    copy.start()
                    copies[way, step, chunk] = copy
    for copy in copies.values():
        copy.wait_send()


def ring_scatter(key_part, value_part, key_raw, gain, number):
    chunks, n, rows, columns = key_part.shape
    out = jax.ShapeDtypeStruct((chunks, rows, columns), BF16)
    sent = 2 * chunks * (n - 1) * rows * columns * 2
    return pl.pallas_call(
        functools.partial(scatter_kernel, n, gain.shape[1]),
        out_shape=(out, out),
        in_specs=[pl.BlockSpec(memory_space=VMEM)] * 4,
        out_specs=(pl.BlockSpec(memory_space=VMEM),) * 2,
        scratch_shapes=[
            pltpu.VMEM((2, n - 1, chunks, rows, columns), BF16),
            pltpu.SemaphoreType.DMA((2, n - 1, chunks)),
            pltpu.SemaphoreType.DMA((2, n - 1, chunks)),
        ],
        compiler_params=pltpu.CompilerParams(collective_id=number, has_side_effects=True),
        cost_estimate=pl.CostEstimate(flops=100_000_000_000 // 4, bytes_accessed=sent, transcendentals=0),
        name="ring_scatter",
    )(key_part, value_part, key_raw, gain)


def norm_kernel(head_dim, raw_ref, gain_ref, out_ref):
    gain = gain_ref[...]
    for at in range(raw_ref.shape[-1] // head_dim):
        cut = slice(at * head_dim, (at + 1) * head_dim)
        raw = raw_ref[:, :, cut]
        out_ref[:, :, cut] = (raw * inverse_of(raw) * gain).astype(BF16)


def attention_kernel(group, tile_tokens, tiles_ref, query_ref, grad_ref, key_ref, value_ref, gain_ref,
                     query_out, key_out, value_out):
    text_rows = query_ref.shape[1]
    head_dim = key_ref.shape[2]
    scale = head_dim ** (-0.5)
    live = tiles_ref[pl.program_id(0)] * tile_tokens

    def stacked(ref):
        return jnp.concatenate(
            [ref[0, :, at * head_dim : (at + 1) * head_dim] for at in range(group)], axis=0
        )

    def mul(left, right, dims):
        return lax.dot_general(left, right, (dims, ((), ())), preferred_element_type=F32)

    raw = stacked(query_ref).astype(F32)
    outs = stacked(grad_ref)
    gain = gain_ref[...]
    inverse = inverse_of(raw)
    normed = (raw * inverse * gain).astype(BF16)
    keys = key_ref[0]
    values = value_ref[0]
    scores = mul(normed, keys, ((1,), (1,))) * scale
    token = lax.broadcasted_iota(jnp.int32, scores.shape, 1)
    scores = jnp.where(token < live, scores, NEG)
    expo = jnp.exp(scores - jnp.max(scores, axis=-1, keepdims=True))
    probs = expo * (1.0 / jnp.sum(expo, axis=-1, keepdims=True))
    probs_b = probs.astype(BF16)
    attn = mul(probs_b, values, ((1,), (0,))).astype(BF16)
    delta = jnp.sum(outs.astype(F32) * attn.astype(F32), axis=-1, keepdims=True)
    dprobs = mul(outs, values, ((1,), (1,)))
    dscores = (probs * (dprobs - delta)).astype(BF16)
    value_out[0] = mul(probs_b, outs, ((0,), (0,))).astype(BF16)
    key_out[0] = (mul(dscores, normed, ((0,), (0,))) * scale).astype(BF16)
    dnormed = mul(dscores, keys, ((1,), (0,))) * scale
    back = norm_back(raw, inverse, gain, dnormed).astype(BF16)
    for at in range(group):
        query_out[0, :, at * head_dim : (at + 1) * head_dim] = back[at * text_rows : (at + 1) * text_rows]


def attention(tiles, queries, out_grad, keys, values, gain):
    samples, text_rows, query_width = queries.shape
    tokens, key_width = keys.shape[1:]
    head_dim = gain.shape[1]
    heads = key_width // head_dim
    group = query_width // key_width
    wide = pl.BlockSpec((1, text_rows, group * head_dim), lambda s, h: (s, 0, h))
    tall = pl.BlockSpec((1, tokens, head_dim), lambda s, h: (s, 0, h))
    flops = samples * query_width * text_rows * tokens * 10
    part = jax.ShapeDtypeStruct((samples, tokens, key_width), BF16)
    return pl.pallas_call(
        functools.partial(attention_kernel, group, tokens // MAX_TILES),
        grid=(samples, heads),
        out_shape=(jax.ShapeDtypeStruct(queries.shape, BF16), part, part),
        in_specs=[
            pl.BlockSpec(memory_space=pltpu.SMEM),
            wide,
            wide,
            tall,
            tall,
            pl.BlockSpec((1, head_dim), lambda s, h: (0, 0)),
        ],
        out_specs=(wide, tall, tall),
        compiler_params=pltpu.CompilerParams(vmem_limit_bytes=48 * 1024 * 1024),
        cost_estimate=pl.CostEstimate(flops=flops, bytes_accessed=8_000_000, transcendentals=0),
        name="attention",
    )(tiles, queries, out_grad, keys, values, gain)


def local(sizes, queries, vision, key_weight, value_weight, query_gain, key_gain, out_grad, tile_count):
    pairs, n, heads_cut = sizes
    head_dim = query_gain.shape[0]
    samples, rows, model_width = vision.shape
    columns = key_weight.shape[1]
    flat_vision = vision.reshape(samples * rows, model_width)

    shard = model_width // (pairs * CHUNKS * n)
    cut = flat_vision.reshape(samples * rows, pairs, CHUNKS, n, shard)
    cut = cut.transpose(1, 3, 0, 2, 4).reshape(pairs * n, samples * rows, CHUNKS * shard)
    column_vision = lax.all_to_all(cut, ("dp", "seq"), split_axis=0, concat_axis=0, tiled=True)
    column_vision = column_vision.reshape(pairs, n, samples, rows, CHUNKS * shard)
    column_vision = column_vision.transpose(0, 2, 1, 3, 4).reshape(-1, CHUNKS * shard)

    key_raw = jnp.dot(flat_vision, key_weight, preferred_element_type=F32)
    key_raw = key_raw.reshape(samples, rows, columns)
    own_values = jnp.dot(flat_vision, value_weight, preferred_element_type=F32).astype(BF16)
    own_values = own_values.reshape(samples, rows, columns)
    own_keys = pl.pallas_call(
        functools.partial(norm_kernel, head_dim),
        out_shape=jax.ShapeDtypeStruct(key_raw.shape, BF16),
        name="key_norm",
    )(key_raw, key_gain[None])
    keys_all, values_all = ring_gather(own_keys, own_values, n, 1, 1)
    keys_all = keys_all.reshape(samples, n * rows, columns)
    values_all = values_all.reshape(samples, n * rows, columns)
    query_grad, key_part, value_part = attention(
        tile_count, queries, out_grad, keys_all, values_all, query_gain[None]
    )
    key_grad, value_grad = ring_scatter(
        key_part.reshape(samples, n, rows, columns),
        value_part.reshape(samples, n, rows, columns),
        key_raw,
        key_gain[None],
        2,
    )

    share = model_width // heads_cut
    vision_part = jnp.einsum(
        "rc,dc->rd", key_grad.reshape(samples * rows, columns), key_weight, preferred_element_type=F32
    ) + jnp.einsum(
        "rc,dc->rd", value_grad.reshape(samples * rows, columns), value_weight, preferred_element_type=F32
    )
    me = lax.axis_index("mp")
    total = lax.dynamic_slice_in_dim(vision_part, me * share, share, axis=1)
    for shift in range(1, heads_cut):
        leaving = lax.dynamic_slice_in_dim(
            vision_part, lax.rem(me + shift, heads_cut) * share, share, axis=1
        ).astype(BF16)
        arrived = lax.ppermute(leaving, "mp", [(at, (at + shift) % heads_cut) for at in range(heads_cut)])
        total = total + arrived.astype(F32)
    vision_grad = total.astype(BF16).reshape(samples, rows, share)

    every_key, every_value = ring_gather(key_grad, value_grad, n, pairs, 3)
    outs = []
    for every in (every_key, every_value):
        grad = jnp.einsum(
            "td,tc->dc", column_vision, every.reshape(-1, columns), preferred_element_type=F32
        )
        outs.append(grad.astype(BF16).reshape(CHUNKS, shard, columns))
    key_rows, value_rows = ring_gather(outs[0], outs[1], n, pairs, 4)
    return (
        query_grad,
        vision_grad,
        key_rows.reshape(model_width, columns).astype(F32),
        value_rows.reshape(model_width, columns).astype(F32),
    )


def solution(mesh):
    sizes = (mesh.shape["dp"], mesh.shape["seq"], mesh.shape["mp"])
    in_specs = (
        P("dp", "seq", "mp"),
        P("dp", "seq", None),
        P(None, "mp"),
        P(None, "mp"),
        P(),
        P(),
        P("dp", "seq", "mp"),
        P("dp"),
    )
    out_specs = (P("dp", "seq", "mp"), P("dp", "seq", "mp"), P(None, "mp"), P(None, "mp"))
    return jax.shard_map(
        functools.partial(local, sizes), mesh=mesh, in_specs=in_specs, out_specs=out_specs, check_vma=False
    )
```

```python
import functools

import jax
import jax.numpy as jnp
from jax import lax
from jax.experimental import pallas as pl
from jax.experimental.pallas import tpu as pltpu
from jax.sharding import PartitionSpec as P

MAX_TILES = 4
EPS = 1e-05
NEG = -1e30
MESH = pl.DeviceIdType.MESH
VMEM = pltpu.VMEM
F32 = jnp.float32
BF16 = jnp.bfloat16


def chunks_of(width, pairs, n):
    return 2 if width % (2 * pairs * n * 128) == 0 else 1


def norm_back(raw, inverse, gain, upstream):
    weighted = upstream * gain
    return inverse * weighted - raw * inverse * inverse * inverse * jnp.mean(
        weighted * raw, axis=-1, keepdims=True
    )


def inverse_of(raw):
    return lax.rsqrt(jnp.mean(raw * raw, axis=-1, keepdims=True) + EPS)


def seq_of(place, n):
    half = place // (n // 2)
    along = place + half * (n - 1 - 2 * place)
    return 2 * along + half


def place_of(index, n):
    side = index % 2
    along = index // 2
    return along + side * (n - 1 - 2 * along)


def ring(n):
    here = lax.axis_index("seq")
    place = place_of(here, n)
    nexts = (seq_of((place + 1) % n, n), seq_of((place + n - 1) % n, n))
    return here, place, nexts


def greet(devices):
    barrier = pltpu.get_barrier_semaphore()
    for device in devices:
        pl.semaphore_signal(barrier, inc=1, device_id=device, device_id_type=MESH)
    pl.semaphore_wait(barrier, len(devices))


def run_ring(n, pairs, sources, outs, sems, prepare=None, jobs=(), kept=True):
    send_sem, recv_sem, pair_send, pair_recv = sems
    here, place, nexts = ring(n)
    lane = lax.axis_index("dp") if pairs > 1 else 0
    chunks = sources[0].shape[0]
    others = [(lane + shift) % pairs for shift in range(1, pairs)]
    ring_copies, pair_copies = {}, []
    jobs = list(jobs)

    def pass_on(way, step, chunk):
        origin = seq_of((place + n - step) % n if way == 0 else (place + step) % n, n)
        target = outs[way].at[lane, chunk, origin] if kept else outs[way].at[chunk, origin]
        block = sources[way].at[chunk] if step == 0 else target
        if step > 0:
            ring_copies[way, step - 1, chunk].wait_recv()
        if step < n - 1:
            copy = pltpu.make_async_remote_copy(
                src_ref=block,
                dst_ref=target,
                send_sem=send_sem.at[way, step, chunk],
                recv_sem=recv_sem.at[way, step, chunk],
                device_id={"seq": nexts[way]},
                device_id_type=MESH,
            )
            copy.start()
            ring_copies[way, step, chunk] = copy
        for at, other in enumerate(others):
            copy = pltpu.make_async_remote_copy(
                src_ref=block,
                dst_ref=target,
                send_sem=pair_send.at[way, step, chunk, at],
                recv_sem=pair_recv.at[way, step, chunk, at],
                device_id={"dp": other},
                device_id_type=MESH,
            )
            copy.start()
            pair_copies.append(copy)

    for way in range(2):
        if prepare is not None:
            prepare(way)
        for chunk in range(chunks):
            pass_on(way, 0, chunk)
    for way in range(2):
        for chunk in range(chunks):
            if kept:
                outs[way][lane, chunk, here] = sources[way][chunk]
            else:
                outs[way][chunk, here] = sources[way][chunk]
    for step in range(1, n):
        for chunk in range(chunks):
            if jobs:
                jobs.pop(0)()
            for way in range(2):
                pass_on(way, step, chunk)
    for job in jobs:
        job()
    for copy in ring_copies.values():
        copy.wait_send()
    for copy in pair_copies:
        copy.wait_send()
        copy.wait_recv()


def ring_sems(n, pairs, chunks):
    return [
        pltpu.SemaphoreType.DMA((2, n, chunks)),
        pltpu.SemaphoreType.DMA((2, n, chunks)),
        pltpu.SemaphoreType.DMA((2, n, chunks, max(pairs - 1, 1))),
        pltpu.SemaphoreType.DMA((2, n, chunks, max(pairs - 1, 1))),
    ]


def greet_ring(n, pairs, mates=()):
    nexts = ring(n)[2]
    lane = lax.axis_index("dp")
    others = [{"dp": (lane + shift) % pairs} for shift in range(1, pairs)]
    greet([{"seq": nexts[0]}, {"seq": nexts[1]}] + others + list(mates))


def size_of(*arrays):
    return sum(array.size * array.dtype.itemsize for array in arrays)


def limit_of(*arrays):
    return size_of(*arrays) + 4 * 1024 * 1024


def cost_of(sent):
    return pl.CostEstimate(flops=25_000_000_000, bytes_accessed=sent, transcendentals=0)


def gather_kernel(n, pairs, first_ref, second_ref, first_out, second_out, *sems):
    greet_ring(n, pairs)
    run_ring(n, pairs, (first_ref, second_ref), (first_out, second_out), sems)


def ring_gather(first, second, n, pairs, number):
    chunks, rows, columns = first.shape
    out = jax.ShapeDtypeStruct((pairs, chunks, n, rows, columns), first.dtype)
    sent = 2 * chunks * (n - 1) * rows * columns * 2
    return pl.pallas_call(
        functools.partial(gather_kernel, n, pairs),
        out_shape=(out, out),
        in_specs=[pl.BlockSpec(memory_space=VMEM)] * 2,
        out_specs=(pl.BlockSpec(memory_space=VMEM),) * 2,
        scratch_shapes=ring_sems(n, pairs, chunks),
        compiler_params=pltpu.CompilerParams(
            collective_id=number, has_side_effects=True, vmem_limit_bytes=limit_of(first, second, out, out)
        ),
        cost_estimate=cost_of(sent),
        name=f"ring_gather_{number}",
    )(first, second)


WEIGHT_CUTS = 4


def project_kernel(sizes, groups, vision_hbm, key_hbm, value_hbm, gain_ref, keys_out, values_out, raw_out,
                   columns_out, vision, key_weight, value_weight, own_keys, own_values, load_sem,
                   push_send, push_recv, own_sem, mate_send, mate_recv, *sems):
    pairs, n, heads_cut = sizes
    samples, rows, width = vision.shape
    columns = key_weight.shape[1]
    head_dim = gain_ref.shape[1]
    shard = columns_out.shape[-1]
    lane, here, me = lax.axis_index("dp"), lax.axis_index("seq"), lax.axis_index("mp")
    place = me % groups
    depth = width // WEIGHT_CUTS
    chunks = columns_out.shape[0]

    loads = [pltpu.make_async_copy(vision_hbm, vision, load_sem.at[0])]
    for at, (source, held) in enumerate(((key_hbm, key_weight), (value_hbm, value_weight))):
        for cut in range(WEIGHT_CUTS):
            span = pl.ds(cut * depth, depth)
            loads.append(
                pltpu.make_async_copy(
                    source.at[span], held.at[span], load_sem.at[1 + at * WEIGHT_CUTS + cut]
                )
            )
    for load in loads:
        load.start()
    shifts = range(1, pairs * n)
    mates = [me - place + (place + shift) % groups for shift in range(1, groups)]
    peers = [((lane + shift // n) % pairs, (here + shift % n) % n) for shift in shifts]
    greet([{"dp": peer[0], "seq": peer[1]} for peer in peers] + [{"mp": mate} for mate in mates])
    loads[0].wait()

    which = [place] if groups > 1 else list(range(samples))
    pushes, own_copies = [], []
    for chunk in range(chunks):
        for at, sample in enumerate(which):
            def columns_of(pair, seat, chunk=chunk, sample=sample):
                start = ((pair * chunks + chunk) * n + seat) * shard
                return vision.at[sample, :, pl.ds(pl.multiple_of(start, shard), shard)]

            target = columns_out.at[chunk, lane, sample, here]
            copy = pltpu.make_async_copy(columns_of(lane, here), target, own_sem.at[chunk, at])
            copy.start()
            own_copies.append(copy)
            for shift, peer in zip(shifts, peers):
                copy = pltpu.make_async_remote_copy(
                    src_ref=columns_of(*peer),
                    dst_ref=target,
                    send_sem=push_send.at[chunk, at, shift],
                    recv_sem=push_recv.at[chunk, at, shift],
                    device_id={"dp": peer[0], "seq": peer[1]},
                    device_id_type=MESH,
                )
                copy.start()
                pushes.append(copy)

    def product(at, weight, cut, total):
        loads[1 + at * WEIGHT_CUTS + cut].wait()
        left = vision[:, :, cut * depth : (cut + 1) * depth].reshape(samples * rows, depth)
        part = jnp.dot(left, weight[cut * depth : (cut + 1) * depth], preferred_element_type=F32)
        return part if total is None else total + part

    state = {}

    def prepare(way):
        if way == 0:
            raw = None
            for cut in range(WEIGHT_CUTS):
                raw = product(0, key_weight, cut, raw)
            for at in range(columns // head_dim):
                span = slice(at * head_dim, (at + 1) * head_dim)
                head = raw[:, span]
                normed = (head * inverse_of(head) * gain_ref[...]).astype(BF16)
                raw_out[:, :, span] = head.reshape(samples, rows, head_dim)
                own_keys[:, :, span] = normed.reshape(samples, rows, head_dim)
            state["values"] = product(1, value_weight, 0, None)
            return
        total = state["values"]
        for cut in range(1, WEIGHT_CUTS):
            total = product(1, value_weight, cut, total)
        own_values[...] = total.astype(BF16).reshape(samples, rows, columns)

    mate_copies = []

    def forward():
        for copy in own_copies:
            copy.wait()
        for copy in pushes:
            copy.wait_recv()
        for at, mate in enumerate(mates):
            for chunk in range(chunks):
                for pair in range(pairs):
                    block = columns_out.at[chunk, pair, place]
                    copy = pltpu.make_async_remote_copy(
                        src_ref=block,
                        dst_ref=block,
                        send_sem=mate_send.at[at, chunk, pair],
                        recv_sem=mate_recv.at[at, chunk, pair],
                        device_id={"mp": mate},
                        device_id_type=MESH,
                    )
                    copy.start()
                    mate_copies.append(copy)

    def idle():
        pass

    jobs = [idle] * 5 + [forward]
    run_ring(n, 1, (own_keys, own_values), (keys_out, values_out), sems, prepare, jobs, kept=False)
    for copy in pushes:
        copy.wait_send()
    for copy in mate_copies:
        copy.wait_send()
        copy.wait_recv()


def project(sizes, vision, key_weight, value_weight, gain):
    pairs, n, heads_cut = sizes
    samples, rows, width = vision.shape
    columns = key_weight.shape[1]
    chunks = chunks_of(width, pairs, n)
    shard = width // (pairs * chunks * n)
    groups = samples if heads_cut % samples == 0 else 1
    each = 1 if groups > 1 else samples
    gathered = jax.ShapeDtypeStruct((samples, n, rows, columns), BF16)
    raw = jax.ShapeDtypeStruct((samples, rows, columns), F32)
    cut = jax.ShapeDtypeStruct((chunks, pairs, samples, n, rows, shard), BF16)
    sent = 2 * samples * (n - 1) * rows * columns * 2 + size_of(cut)
    dma = pltpu.SemaphoreType.DMA
    own = pltpu.VMEM((samples, rows, columns), BF16)
    return pl.pallas_call(
        functools.partial(project_kernel, sizes, groups),
        out_shape=(gathered, gathered, raw, cut),
        in_specs=[pl.BlockSpec(memory_space=pl.ANY)] * 3 + [pl.BlockSpec(memory_space=VMEM)],
        out_specs=(pl.BlockSpec(memory_space=VMEM),) * 4,
        scratch_shapes=[
            pltpu.VMEM(vision.shape, BF16),
            pltpu.VMEM(key_weight.shape, BF16),
            pltpu.VMEM(value_weight.shape, BF16),
            own,
            own,
            dma((1 + 2 * WEIGHT_CUTS,)),
            dma((chunks, each, pairs * n)),
            dma((chunks, each, pairs * n)),
            dma((chunks, each)),
            dma((max(groups - 1, 1), chunks, pairs)),
            dma((max(groups - 1, 1), chunks, pairs)),
        ]
        + ring_sems(n, 1, samples),
        compiler_params=pltpu.CompilerParams(
            collective_id=1,
            has_side_effects=True,
            vmem_limit_bytes=limit_of(vision, key_weight, value_weight, gathered, gathered, raw, raw, cut),
        ),
        cost_estimate=cost_of(sent),
        name="project_gather",
    )(vision, key_weight, value_weight, gain)


def vision_kernel(sizes, tile, key_ref, value_ref, key_hbm, value_hbm, key_out, value_out, vision_out,
                  key_weight, value_weight, leaving, arrived, total, load_sem, leave_sem, arrive_sem, *sems):
    pairs, n, heads_cut = sizes
    me = lax.axis_index("mp")
    loads = [
        pltpu.make_async_copy(key_hbm, key_weight, load_sem.at[0]),
        pltpu.make_async_copy(value_hbm, value_weight, load_sem.at[1]),
    ]
    for load in loads:
        load.start()
    mates = [(me + shift) % heads_cut for shift in range(1, heads_cut)]
    greet_ring(n, pairs, [{"mp": mate} for mate in mates])
    share = total.shape[1]
    columns = key_ref.shape[-1]
    tiles = share // tile
    copies = []

    def compute(owner, at, store):
        span = pl.ds(pl.multiple_of(owner * share + at * tile, tile), tile)
        part = None
        for ref, weight in ((key_ref, key_weight), (value_ref, value_weight)):
            left = ref[...].reshape(total.shape[0], columns)
            term = lax.dot_general(
                left, weight[span, :], (((1,), (1,)), ((), ())), preferred_element_type=F32
            )
            part = term if part is None else part + term
        store(part)

    def load_all():
        for load in loads:
            load.wait()

    def leave(at):
        copy = pltpu.make_async_remote_copy(
            src_ref=leaving.at[at],
            dst_ref=arrived.at[at],
            send_sem=leave_sem.at[at],
            recv_sem=arrive_sem.at[at],
            device_id={"mp": mates[at]},
            device_id_type=MESH,
        )
        copy.start()
        copies.append(copy)

    jobs = [load_all]
    waiting = None
    for turn, owner in enumerate(mates + [me]):
        for at in range(tiles):
            span = slice(at * tile, (at + 1) * tile)

            def job(turn=turn, owner=owner, at=at, span=span, due=waiting):
                def store(part):
                    if turn < len(mates):
                        leaving[turn, :, span] = part.astype(BF16)
                    else:
                        total[:, span] = part

                compute(owner, at, store)
                if due is not None:
                    leave(due)

            jobs.append(job)
            waiting = None
        waiting = turn
    run_ring(n, pairs, (key_ref, value_ref), (key_out, value_out), sems, None, jobs)
    result = total[...]
    for at, copy in enumerate(copies):
        copy.wait()
        result = result + arrived[at].astype(F32)
    vision_out[...] = result.astype(BF16)


def vision_gather(sizes, key_grad, value_grad, key_weight, value_weight):
    pairs, n, heads_cut = sizes
    samples, rows, columns = key_grad.shape
    share = key_weight.shape[0] // heads_cut
    tile = 512 if share % 512 == 0 else share
    out = jax.ShapeDtypeStruct((pairs, samples, n, rows, columns), BF16)
    vision = jax.ShapeDtypeStruct((samples * rows, share), BF16)
    moved = jax.ShapeDtypeStruct((max(heads_cut - 1, 1), samples * rows, share), BF16)
    sent = 2 * samples * (n - 1) * rows * columns * 2
    dma = pltpu.SemaphoreType.DMA
    total = jax.ShapeDtypeStruct((samples * rows, share), F32)
    return pl.pallas_call(
        functools.partial(vision_kernel, sizes, tile),
        out_shape=(out, out, vision),
        in_specs=[pl.BlockSpec(memory_space=VMEM)] * 2 + [pl.BlockSpec(memory_space=pl.ANY)] * 2,
        out_specs=(pl.BlockSpec(memory_space=VMEM),) * 3,
        scratch_shapes=[
            pltpu.VMEM(key_weight.shape, BF16),
            pltpu.VMEM(value_weight.shape, BF16),
            pltpu.VMEM(moved.shape, BF16),
            pltpu.VMEM(moved.shape, BF16),
            pltpu.VMEM(total.shape, F32),
            dma((2,)),
            dma((max(heads_cut - 1, 1),)),
            dma((max(heads_cut - 1, 1),)),
        ]
        + ring_sems(n, pairs, samples),
        compiler_params=pltpu.CompilerParams(
            collective_id=3,
            has_side_effects=True,
            vmem_limit_bytes=limit_of(
                key_grad, value_grad, key_weight, value_weight, moved, moved, total, total, out, out, vision
            ),
        ),
        cost_estimate=cost_of(sent),
        name="vision_gather",
    )(key_grad, value_grad, key_weight, value_weight)


def scatter_kernel(n, head_dim, key_ref, value_ref, raw_ref, gain_ref, key_out, value_out, *scratch):
    held, send_sem, recv_sem = scratch
    parts = (key_ref, value_ref)
    here, place, nexts = ring(n)
    chunks = key_ref.shape[0]
    greet([{"seq": nexts[0]}, {"seq": nexts[1]}])

    def copy_of(way, step, chunk, block):
        return pltpu.make_async_remote_copy(
            src_ref=block,
            dst_ref=held.at[way, step, chunk],
            send_sem=send_sem.at[way, step, chunk],
            recv_sem=recv_sem.at[way, step, chunk],
            device_id={"seq": nexts[way]},
            device_id_type=MESH,
        )

    def dest_of(way, step):
        if way == 0:
            return seq_of((place + 2 * n - 1 - step) % n, n)
        return seq_of((place + 1 + step) % n, n)

    copies = {}
    for chunk in range(chunks):
        for way in range(2):
            copy = copy_of(way, 0, chunk, parts[way].at[chunk, dest_of(way, 0)])
            copy.start()
            copies[way, 0, chunk] = copy
    for step in range(1, n):
        for chunk in range(chunks):
            for way in range(2):
                copies[way, step - 1, chunk].wait_recv()
                own = parts[way][chunk, dest_of(way, step)].astype(F32)
                total = held[way, step - 1, chunk].astype(F32) + own
                if step < n - 1:
                    held[way, step - 1, chunk] = total.astype(BF16)
                elif way == 1:
                    value_out[chunk] = total.astype(BF16)
                else:
                    gain = gain_ref[...]
                    for at in range(total.shape[1] // head_dim):
                        cut = slice(at * head_dim, (at + 1) * head_dim)
                        raw = raw_ref[chunk, :, cut]
                        grad = norm_back(raw, inverse_of(raw), gain, total[:, cut])
                        key_out[chunk, :, cut] = grad.astype(BF16)
            if step < n - 1:
                for way in range(2):
                    copy = copy_of(way, step, chunk, held.at[way, step - 1, chunk])
                    copy.start()
                    copies[way, step, chunk] = copy
    for copy in copies.values():
        copy.wait_send()


def ring_scatter(key_part, value_part, key_raw, gain, number):
    chunks, n, rows, columns = key_part.shape
    out = jax.ShapeDtypeStruct((chunks, rows, columns), BF16)
    sent = 2 * chunks * (n - 1) * rows * columns * 2
    return pl.pallas_call(
        functools.partial(scatter_kernel, n, gain.shape[1]),
        out_shape=(out, out),
        in_specs=[pl.BlockSpec(memory_space=VMEM)] * 4,
        out_specs=(pl.BlockSpec(memory_space=VMEM),) * 2,
        scratch_shapes=[
            pltpu.VMEM((2, n - 1, chunks, rows, columns), BF16),
            pltpu.SemaphoreType.DMA((2, n - 1, chunks)),
            pltpu.SemaphoreType.DMA((2, n - 1, chunks)),
        ],
        compiler_params=pltpu.CompilerParams(
            collective_id=number,
            has_side_effects=True,
            vmem_limit_bytes=limit_of(key_part, value_part, key_part, value_part, key_raw, out, out),
        ),
        cost_estimate=cost_of(sent),
        name="ring_scatter",
    )(key_part, value_part, key_raw, gain)


def attention_kernel(group, tile_tokens, tiles_ref, query_ref, grad_ref, key_ref, value_ref, gain_ref,
                     query_out, key_out, value_out):
    text_rows = query_ref.shape[1]
    head_dim = key_ref.shape[2]
    scale = head_dim ** (-0.5)
    live = tiles_ref[pl.program_id(0)] * tile_tokens

    def stacked(ref):
        return jnp.concatenate(
            [ref[0, :, at * head_dim : (at + 1) * head_dim] for at in range(group)], axis=0
        )

    def mul(left, right, dims):
        return lax.dot_general(left, right, (dims, ((), ())), preferred_element_type=F32)

    raw = stacked(query_ref).astype(F32)
    outs = stacked(grad_ref)
    gain = gain_ref[...]
    inverse = inverse_of(raw)
    normed = (raw * inverse * gain).astype(BF16)
    keys = key_ref[0]
    values = value_ref[0]
    scores = mul(normed, keys, ((1,), (1,))) * scale
    token = lax.broadcasted_iota(jnp.int32, scores.shape, 1)
    scores = jnp.where(token < live, scores, NEG)
    expo = jnp.exp(scores - jnp.max(scores, axis=-1, keepdims=True))
    probs = expo * (1.0 / jnp.sum(expo, axis=-1, keepdims=True))
    probs_b = probs.astype(BF16)
    attn = mul(probs_b, values, ((1,), (0,))).astype(BF16)
    delta = jnp.sum(outs.astype(F32) * attn.astype(F32), axis=-1, keepdims=True)
    dprobs = mul(outs, values, ((1,), (1,)))
    dscores = (probs * (dprobs - delta)).astype(BF16)
    value_out[0] = mul(probs_b, outs, ((0,), (0,))).astype(BF16)
    key_out[0] = (mul(dscores, normed, ((0,), (0,))) * scale).astype(BF16)
    dnormed = mul(dscores, keys, ((1,), (0,))) * scale
    back = norm_back(raw, inverse, gain, dnormed).astype(BF16)
    for at in range(group):
        query_out[0, :, at * head_dim : (at + 1) * head_dim] = back[at * text_rows : (at + 1) * text_rows]


def attention(tiles, queries, out_grad, keys, values, gain):
    samples, text_rows, query_width = queries.shape
    tokens, key_width = keys.shape[1:]
    head_dim = gain.shape[1]
    heads = key_width // head_dim
    group = query_width // key_width
    wide = pl.BlockSpec((1, text_rows, group * head_dim), lambda s, h: (s, 0, h))
    tall = pl.BlockSpec((1, tokens, head_dim), lambda s, h: (s, 0, h))
    flops = samples * query_width * text_rows * tokens * 10
    part = jax.ShapeDtypeStruct((samples, tokens, key_width), BF16)
    return pl.pallas_call(
        functools.partial(attention_kernel, group, tokens // MAX_TILES),
        grid=(samples, heads),
        out_shape=(jax.ShapeDtypeStruct(queries.shape, BF16), part, part),
        in_specs=[
            pl.BlockSpec(memory_space=pltpu.SMEM),
            wide,
            wide,
            tall,
            tall,
            pl.BlockSpec((1, head_dim), lambda s, h: (0, 0)),
        ],
        out_specs=(wide, tall, tall),
        compiler_params=pltpu.CompilerParams(vmem_limit_bytes=48 * 1024 * 1024),
        cost_estimate=pl.CostEstimate(flops=flops, bytes_accessed=8_000_000, transcendentals=0),
        name="attention",
    )(tiles, queries, out_grad, keys, values, gain)


def local(sizes, queries, vision, key_weight, value_weight, query_gain, key_gain, out_grad, tile_count):
    pairs, n, heads_cut = sizes
    samples, rows, model_width = vision.shape
    columns = key_weight.shape[1]
    keys_all, values_all, key_raw, column_vision = project(
        sizes, vision, key_weight, value_weight, key_gain[None]
    )
    query_grad, key_part, value_part = attention(
        tile_count,
        queries,
        out_grad,
        keys_all.reshape(samples, n * rows, columns),
        values_all.reshape(samples, n * rows, columns),
        query_gain[None],
    )
    key_grad, value_grad = ring_scatter(
        key_part.reshape(samples, n, rows, columns),
        value_part.reshape(samples, n, rows, columns),
        key_raw,
        key_gain[None],
        2,
    )
    every_key, every_value, vision_grad = vision_gather(
        sizes, key_grad, value_grad, key_weight, value_weight
    )
    tokens = pairs * samples * n * rows
    column_vision = column_vision.reshape(column_vision.shape[0], tokens, -1)
    outs = []
    for every in (every_key, every_value):
        grad = jnp.einsum(
            "ktd,tc->kdc", column_vision, every.reshape(tokens, columns), preferred_element_type=F32
        )
        outs.append(grad.astype(BF16))
    key_rows, value_rows = ring_gather(outs[0], outs[1], n, pairs, 4)
    return (
        query_grad,
        vision_grad.reshape(samples, rows, -1),
        key_rows.reshape(model_width, columns).astype(F32),
        value_rows.reshape(model_width, columns).astype(F32),
    )


def solution(mesh):
    sizes = (mesh.shape["dp"], mesh.shape["seq"], mesh.shape["mp"])
    in_specs = (
        P("dp", "seq", "mp"),
        P("dp", "seq", None),
        P(None, "mp"),
        P(None, "mp"),
        P(),
        P(),
        P("dp", "seq", "mp"),
        P("dp"),
    )
    out_specs = (P("dp", "seq", "mp"), P("dp", "seq", "mp"), P(None, "mp"), P(None, "mp"))
    return jax.shard_map(
        functools.partial(local, sizes), mesh=mesh, in_specs=in_specs, out_specs=out_specs, check_vma=False
    )
```

```python
import functools

import jax
import jax.numpy as jnp
from jax import lax
from jax.experimental import pallas as pl
from jax.experimental.pallas import tpu as pltpu
from jax.sharding import PartitionSpec as P

MAX_TILES = 4
EPS = 1e-05
NEG = -1e30
MESH = pl.DeviceIdType.MESH
VMEM = pltpu.VMEM
F32 = jnp.float32
BF16 = jnp.bfloat16


def chunks_of(width, pairs, n):
    return 2 if width % (2 * pairs * n * 128) == 0 else 1


def norm_back(raw, inverse, gain, upstream):
    weighted = upstream * gain
    return inverse * weighted - raw * inverse * inverse * inverse * jnp.mean(
        weighted * raw, axis=-1, keepdims=True
    )


def inverse_of(raw):
    return lax.rsqrt(jnp.mean(raw * raw, axis=-1, keepdims=True) + EPS)


def seq_of(place, n):
    half = place // (n // 2)
    along = place + half * (n - 1 - 2 * place)
    return 2 * along + half


def place_of(index, n):
    side = index % 2
    along = index // 2
    return along + side * (n - 1 - 2 * along)


def ring(n):
    here = lax.axis_index("seq")
    place = place_of(here, n)
    nexts = (seq_of((place + 1) % n, n), seq_of((place + n - 1) % n, n))
    return here, place, nexts


def greet(devices):
    barrier = pltpu.get_barrier_semaphore()
    for device in devices:
        pl.semaphore_signal(barrier, inc=1, device_id=device, device_id_type=MESH)
    pl.semaphore_wait(barrier, len(devices))


def run_ring(n, pairs, sources, outs, sems, prepare=None, jobs=(), kept=True):
    send_sem, recv_sem, pair_send, pair_recv = sems
    here, place, nexts = ring(n)
    lane = lax.axis_index("dp") if pairs > 1 else 0
    chunks = sources[0].shape[0]
    others = [(lane + shift) % pairs for shift in range(1, pairs)]
    ring_copies, pair_copies = {}, []
    jobs = list(jobs)

    def pass_on(way, step, chunk):
        origin = seq_of((place + n - step) % n if way == 0 else (place + step) % n, n)
        target = outs[way].at[lane, chunk, origin] if kept else outs[way].at[chunk, origin]
        block = sources[way].at[chunk] if step == 0 else target
        if step > 0:
            ring_copies[way, step - 1, chunk].wait_recv()
        if step < n - 1:
            copy = pltpu.make_async_remote_copy(
                src_ref=block,
                dst_ref=target,
                send_sem=send_sem.at[way, step, chunk],
                recv_sem=recv_sem.at[way, step, chunk],
                device_id={"seq": nexts[way]},
                device_id_type=MESH,
            )
            copy.start()
            ring_copies[way, step, chunk] = copy
        for at, other in enumerate(others):
            copy = pltpu.make_async_remote_copy(
                src_ref=block,
                dst_ref=target,
                send_sem=pair_send.at[way, step, chunk, at],
                recv_sem=pair_recv.at[way, step, chunk, at],
                device_id={"dp": other},
                device_id_type=MESH,
            )
            copy.start()
            pair_copies.append(copy)

    for way in range(2):
        if prepare is not None:
            prepare(way)
        for chunk in range(chunks):
            pass_on(way, 0, chunk)
    for way in range(2):
        for chunk in range(chunks):
            if kept:
                outs[way][lane, chunk, here] = sources[way][chunk]
            else:
                outs[way][chunk, here] = sources[way][chunk]
    for step in range(1, n):
        for chunk in range(chunks):
            if jobs:
                jobs.pop(0)()
            for way in range(2):
                pass_on(way, step, chunk)
    for job in jobs:
        job()
    for copy in ring_copies.values():
        copy.wait_send()
    for copy in pair_copies:
        copy.wait_send()
        copy.wait_recv()


def ring_sems(n, pairs, chunks):
    return [
        pltpu.SemaphoreType.DMA((2, n, chunks)),
        pltpu.SemaphoreType.DMA((2, n, chunks)),
        pltpu.SemaphoreType.DMA((2, n, chunks, max(pairs - 1, 1))),
        pltpu.SemaphoreType.DMA((2, n, chunks, max(pairs - 1, 1))),
    ]


def greet_ring(n, pairs, mates=()):
    nexts = ring(n)[2]
    lane = lax.axis_index("dp")
    others = [{"dp": (lane + shift) % pairs} for shift in range(1, pairs)]
    greet([{"seq": nexts[0]}, {"seq": nexts[1]}] + others + list(mates))


def size_of(*arrays):
    return sum(array.size * array.dtype.itemsize for array in arrays)


def limit_of(*arrays):
    return size_of(*arrays) + 4 * 1024 * 1024


def cost_of(sent):
    return pl.CostEstimate(flops=25_000_000_000, bytes_accessed=sent, transcendentals=0)


def gather_kernel(n, pairs, first_ref, second_ref, first_out, second_out, *sems):
    greet_ring(n, pairs)
    run_ring(n, pairs, (first_ref, second_ref), (first_out, second_out), sems)


def ring_gather(first, second, n, pairs, number):
    chunks, rows, columns = first.shape
    out = jax.ShapeDtypeStruct((pairs, chunks, n, rows, columns), first.dtype)
    sent = 2 * chunks * (n - 1) * rows * columns * 2
    return pl.pallas_call(
        functools.partial(gather_kernel, n, pairs),
        out_shape=(out, out),
        in_specs=[pl.BlockSpec(memory_space=VMEM)] * 2,
        out_specs=(pl.BlockSpec(memory_space=VMEM),) * 2,
        scratch_shapes=ring_sems(n, pairs, chunks),
        compiler_params=pltpu.CompilerParams(
            collective_id=number, has_side_effects=True, vmem_limit_bytes=limit_of(first, second, out, out)
        ),
        cost_estimate=cost_of(sent),
        name=f"ring_gather_{number}",
    )(first, second)


WEIGHT_CUTS = 4


def project_kernel(sizes, vision_hbm, key_hbm, value_hbm, gain_ref, keys_out, values_out, raw_out,
                   vision, key_weight, value_weight, own_keys, own_values, load_sem, *sems):
    pairs, n, heads_cut = sizes
    samples, rows, width = vision.shape
    columns = key_weight.shape[1]
    head_dim = gain_ref.shape[1]
    depth = width // WEIGHT_CUTS

    loads = [pltpu.make_async_copy(vision_hbm, vision, load_sem.at[0])]
    for at, (source, held) in enumerate(((key_hbm, key_weight), (value_hbm, value_weight))):
        for cut in range(WEIGHT_CUTS):
            span = pl.ds(cut * depth, depth)
            loads.append(
                pltpu.make_async_copy(
                    source.at[span], held.at[span], load_sem.at[1 + at * WEIGHT_CUTS + cut]
                )
            )
    for load in loads:
        load.start()
    greet_ring(n, 1)
    loads[0].wait()

    def product(at, weight, cut, total):
        loads[1 + at * WEIGHT_CUTS + cut].wait()
        left = vision[:, :, cut * depth : (cut + 1) * depth].reshape(samples * rows, depth)
        part = jnp.dot(left, weight[cut * depth : (cut + 1) * depth], preferred_element_type=F32)
        return part if total is None else total + part

    state = {}

    def prepare(way):
        if way == 0:
            raw = None
            for cut in range(WEIGHT_CUTS):
                raw = product(0, key_weight, cut, raw)
            for at in range(columns // head_dim):
                span = slice(at * head_dim, (at + 1) * head_dim)
                head = raw[:, span]
                normed = (head * inverse_of(head) * gain_ref[...]).astype(BF16)
                raw_out[:, :, span] = head.reshape(samples, rows, head_dim)
                own_keys[:, :, span] = normed.reshape(samples, rows, head_dim)
            state["values"] = product(1, value_weight, 0, None)
            return
        total = state["values"]
        for cut in range(1, WEIGHT_CUTS):
            total = product(1, value_weight, cut, total)
        own_values[...] = total.astype(BF16).reshape(samples, rows, columns)

    run_ring(n, 1, (own_keys, own_values), (keys_out, values_out), sems, prepare, kept=False)


def project(sizes, vision, key_weight, value_weight, gain):
    pairs, n, heads_cut = sizes
    samples, rows, width = vision.shape
    columns = key_weight.shape[1]
    gathered = jax.ShapeDtypeStruct((samples, n, rows, columns), BF16)
    raw = jax.ShapeDtypeStruct((samples, rows, columns), F32)
    sent = 2 * samples * (n - 1) * rows * columns * 2
    dma = pltpu.SemaphoreType.DMA
    own = pltpu.VMEM((samples, rows, columns), BF16)
    return pl.pallas_call(
        functools.partial(project_kernel, sizes),
        out_shape=(gathered, gathered, raw),
        in_specs=[pl.BlockSpec(memory_space=pltpu.HBM)] * 3 + [pl.BlockSpec(memory_space=VMEM)],
        out_specs=(pl.BlockSpec(memory_space=VMEM),) * 3,
        scratch_shapes=[
            pltpu.VMEM(vision.shape, BF16),
            pltpu.VMEM(key_weight.shape, BF16),
            pltpu.VMEM(value_weight.shape, BF16),
            own,
            own,
            dma((1 + 2 * WEIGHT_CUTS,)),
        ]
        + ring_sems(n, 1, samples),
        compiler_params=pltpu.CompilerParams(
            collective_id=1,
            has_side_effects=True,
            vmem_limit_bytes=60 * 1024 * 1024,
        ),
        cost_estimate=cost_of(sent),
        name="project_gather",
    )(vision, key_weight, value_weight, gain)


def vision_kernel(sizes, tile, key_ref, value_ref, key_hbm, value_hbm, key_out, value_out, vision_out,
                  key_weight, value_weight, leaving, arrived, total, load_sem, leave_sem, arrive_sem, *sems):
    pairs, n, heads_cut = sizes
    me = lax.axis_index("mp")
    loads = [
        pltpu.make_async_copy(key_hbm, key_weight, load_sem.at[0]),
        pltpu.make_async_copy(value_hbm, value_weight, load_sem.at[1]),
    ]
    for load in loads:
        load.start()
    mates = [(me + shift) % heads_cut for shift in range(1, heads_cut)]
    greet_ring(n, pairs, [{"mp": mate} for mate in mates])
    share = total.shape[1]
    columns = key_ref.shape[-1]
    tiles = share // tile
    copies = []

    def compute(owner, at, store):
        span = pl.ds(pl.multiple_of(owner * share + at * tile, tile), tile)
        part = None
        for ref, weight in ((key_ref, key_weight), (value_ref, value_weight)):
            left = ref[...].reshape(total.shape[0], columns)
            term = lax.dot_general(
                left, weight[span, :], (((1,), (1,)), ((), ())), preferred_element_type=F32
            )
            part = term if part is None else part + term
        store(part)

    def load_all():
        for load in loads:
            load.wait()

    def leave(at):
        copy = pltpu.make_async_remote_copy(
            src_ref=leaving.at[at],
            dst_ref=arrived.at[at],
            send_sem=leave_sem.at[at],
            recv_sem=arrive_sem.at[at],
            device_id={"mp": mates[at]},
            device_id_type=MESH,
        )
        copy.start()
        copies.append(copy)

    jobs = [load_all]
    waiting = None
    for turn, owner in enumerate(mates + [me]):
        for at in range(tiles):
            span = slice(at * tile, (at + 1) * tile)

            def job(turn=turn, owner=owner, at=at, span=span, due=waiting):
                def store(part):
                    if turn < len(mates):
                        leaving[turn, :, span] = part.astype(BF16)
                    else:
                        total[:, span] = part

                compute(owner, at, store)
                if due is not None:
                    leave(due)

            jobs.append(job)
            waiting = None
        waiting = turn
    run_ring(n, pairs, (key_ref, value_ref), (key_out, value_out), sems, None, jobs)
    result = total[...]
    for at, copy in enumerate(copies):
        copy.wait()
        result = result + arrived[at].astype(F32)
    vision_out[...] = result.astype(BF16)


def vision_gather(sizes, key_grad, value_grad, key_weight, value_weight):
    pairs, n, heads_cut = sizes
    samples, rows, columns = key_grad.shape
    share = key_weight.shape[0] // heads_cut
    tile = 512 if share % 512 == 0 else share
    out = jax.ShapeDtypeStruct((pairs, samples, n, rows, columns), BF16)
    vision = jax.ShapeDtypeStruct((samples * rows, share), BF16)
    moved = jax.ShapeDtypeStruct((max(heads_cut - 1, 1), samples * rows, share), BF16)
    sent = 2 * samples * (n - 1) * rows * columns * 2
    dma = pltpu.SemaphoreType.DMA
    total = jax.ShapeDtypeStruct((samples * rows, share), F32)
    return pl.pallas_call(
        functools.partial(vision_kernel, sizes, tile),
        out_shape=(out, out, vision),
        in_specs=[pl.BlockSpec(memory_space=VMEM)] * 2 + [pl.BlockSpec(memory_space=pltpu.HBM)] * 2,
        out_specs=(pl.BlockSpec(memory_space=VMEM),) * 3,
        scratch_shapes=[
            pltpu.VMEM(key_weight.shape, BF16),
            pltpu.VMEM(value_weight.shape, BF16),
            pltpu.VMEM(moved.shape, BF16),
            pltpu.VMEM(moved.shape, BF16),
            pltpu.VMEM(total.shape, F32),
            dma((2,)),
            dma((max(heads_cut - 1, 1),)),
            dma((max(heads_cut - 1, 1),)),
        ]
        + ring_sems(n, pairs, samples),
        compiler_params=pltpu.CompilerParams(
            collective_id=3,
            has_side_effects=True,
            vmem_limit_bytes=limit_of(
                key_grad, value_grad, key_weight, value_weight, moved, moved, total, total, out, out, vision
            ),
        ),
        cost_estimate=cost_of(sent),
        name="vision_gather",
    )(key_grad, value_grad, key_weight, value_weight)


def scatter_kernel(n, groups, head_dim, key_ref, value_ref, raw_ref, gain_ref, half_ref, key_out, value_out,
                   columns_out, held, send_sem, recv_sem, own_sem, mate_send, mate_recv):
    parts = (key_ref, value_ref)
    here, place, nexts = ring(n)
    chunks = key_ref.shape[0]
    me = lax.axis_index("mp")
    seat = me % groups
    mates = [me - seat + (seat + shift) % groups for shift in range(1, groups)]
    greet([{"seq": nexts[0]}, {"seq": nexts[1]}] + [{"mp": mate} for mate in mates])

    def copy_of(way, step, chunk, block):
        return pltpu.make_async_remote_copy(
            src_ref=block,
            dst_ref=held.at[way, step, chunk],
            send_sem=send_sem.at[way, step, chunk],
            recv_sem=recv_sem.at[way, step, chunk],
            device_id={"seq": nexts[way]},
            device_id_type=MESH,
        )

    def dest_of(way, step):
        if way == 0:
            return seq_of((place + 2 * n - 1 - step) % n, n)
        return seq_of((place + 1 + step) % n, n)

    copies = {}
    for chunk in range(chunks):
        for way in range(2):
            copy = copy_of(way, 0, chunk, parts[way].at[chunk, dest_of(way, 0)])
            copy.start()
            copies[way, 0, chunk] = copy
    moved = []
    for cut in range(half_ref.shape[0]):
        for pair in range(half_ref.shape[1]):
            for at in range(half_ref.shape[2]):
                block = half_ref.at[cut, pair, at]
                target = columns_out.at[cut, pair, seat if groups > 1 else at]
                moved.append(pltpu.make_async_copy(block, target, own_sem.at[cut, pair, at]))
                for turn, mate in enumerate(mates):
                    moved.append(
                        pltpu.make_async_remote_copy(
                            src_ref=block,
                            dst_ref=target,
                            send_sem=mate_send.at[cut, pair, turn],
                            recv_sem=mate_recv.at[cut, pair, turn],
                            device_id={"mp": mate},
                            device_id_type=MESH,
                        )
                    )
    for copy in moved:
        copy.start()
    for step in range(1, n):
        for chunk in range(chunks):
            for way in range(2):
                copies[way, step - 1, chunk].wait_recv()
                own = parts[way][chunk, dest_of(way, step)].astype(F32)
                total = held[way, step - 1, chunk].astype(F32) + own
                if step < n - 1:
                    held[way, step - 1, chunk] = total.astype(BF16)
                elif way == 1:
                    value_out[chunk] = total.astype(BF16)
                else:
                    gain = gain_ref[...]
                    for at in range(total.shape[1] // head_dim):
                        cut = slice(at * head_dim, (at + 1) * head_dim)
                        raw = raw_ref[chunk, :, cut]
                        grad = norm_back(raw, inverse_of(raw), gain, total[:, cut])
                        key_out[chunk, :, cut] = grad.astype(BF16)
            if step < n - 1:
                for way in range(2):
                    copy = copy_of(way, step, chunk, held.at[way, step - 1, chunk])
                    copy.start()
                    copies[way, step, chunk] = copy
    for copy in copies.values():
        copy.wait_send()
    for copy in moved:
        copy.wait()


def ring_scatter(sizes, key_part, value_part, key_raw, gain, half, number):
    chunks, n, rows, columns = key_part.shape
    groups = chunks if sizes[2] % chunks == 0 else 1
    cuts, pairs, each = half.shape[:3]
    full = jax.ShapeDtypeStruct((cuts, pairs, chunks) + half.shape[3:], BF16)
    dma = pltpu.SemaphoreType.DMA
    out = jax.ShapeDtypeStruct((chunks, rows, columns), BF16)
    sent = 2 * chunks * (n - 1) * rows * columns * 2
    return pl.pallas_call(
        functools.partial(scatter_kernel, n, groups, gain.shape[1]),
        out_shape=(out, out, full),
        in_specs=[pl.BlockSpec(memory_space=VMEM)] * 5,
        out_specs=(pl.BlockSpec(memory_space=VMEM),) * 3,
        scratch_shapes=[
            pltpu.VMEM((2, n - 1, chunks, rows, columns), BF16),
            dma((2, n - 1, chunks)),
            dma((2, n - 1, chunks)),
            dma((cuts, pairs, each)),
            dma((cuts, pairs, max(groups - 1, 1))),
            dma((cuts, pairs, max(groups - 1, 1))),
        ],
        compiler_params=pltpu.CompilerParams(
            collective_id=number,
            has_side_effects=True,
            vmem_limit_bytes=limit_of(key_part, value_part, key_part, value_part, key_raw, out, out, half, full),
        ),
        cost_estimate=cost_of(sent),
        name="ring_scatter",
    )(key_part, value_part, key_raw, gain, half)


def exchange(sizes, groups, vision, columns_out, push_send, push_recv, own_sem):
    pairs, n, _ = sizes
    chunks, each, shard = columns_out.shape[0], columns_out.shape[2], columns_out.shape[-1]
    lane, here, me = lax.axis_index("dp"), lax.axis_index("seq"), lax.axis_index("mp")
    peers = [((lane + shift // n) % pairs, (here + shift % n) % n) for shift in range(1, pairs * n)]
    own, pushes = [], []
    for chunk in range(chunks):
        for at in range(each):
            sample = me % groups if groups > 1 else at

            def columns_of(pair, seat, chunk=chunk, sample=sample):
                start = ((pair * chunks + chunk) * n + seat) * shard
                return vision.at[sample, :, pl.ds(pl.multiple_of(start, shard), shard)]

            target = columns_out.at[chunk, lane, at, here]
            own.append(pltpu.make_async_copy(columns_of(lane, here), target, own_sem.at[chunk, at]))
            for shift, peer in enumerate(peers):
                pushes.append(
                    pltpu.make_async_remote_copy(
                        src_ref=columns_of(*peer),
                        dst_ref=target,
                        send_sem=push_send.at[chunk, at, shift],
                        recv_sem=push_recv.at[chunk, at, shift],
                        device_id={"dp": peer[0], "seq": peer[1]},
                        device_id_type=MESH,
                    )
                )
    return peers, own + pushes


def attention_kernel(sizes, groups, group, tile_tokens, tiles_ref, query_ref, grad_ref, key_ref, value_ref,
                     gain_ref, vision, query_out, key_out, value_out, columns_out, *sems):
    at_sample, at_head = pl.program_id(0), pl.program_id(1)
    heads = pl.num_programs(1)
    turn = at_sample * heads + at_head

    @pl.when(turn == 0)
    def _():
        peers, copies = exchange(sizes, groups, vision, columns_out, *sems)
        greet([{"dp": peer[0], "seq": peer[1]} for peer in peers])
        for copy in copies:
            copy.start()

    text_rows = query_ref.shape[1]
    head_dim = key_ref.shape[2]
    scale = head_dim ** (-0.5)
    live = tiles_ref[pl.program_id(0)] * tile_tokens

    def stacked(ref):
        return jnp.concatenate(
            [ref[0, :, at * head_dim : (at + 1) * head_dim] for at in range(group)], axis=0
        )

    def mul(left, right, dims):
        return lax.dot_general(left, right, (dims, ((), ())), preferred_element_type=F32)

    raw = stacked(query_ref).astype(F32)
    outs = stacked(grad_ref)
    gain = gain_ref[...]
    inverse = inverse_of(raw)
    normed = (raw * inverse * gain).astype(BF16)
    keys = key_ref[0]
    values = value_ref[0]
    scores = mul(normed, keys, ((1,), (1,))) * scale
    token = lax.broadcasted_iota(jnp.int32, scores.shape, 1)
    scores = jnp.where(token < live, scores, NEG)
    expo = jnp.exp(scores - jnp.max(scores, axis=-1, keepdims=True))
    probs = expo * (1.0 / jnp.sum(expo, axis=-1, keepdims=True))
    probs_b = probs.astype(BF16)
    attn = mul(probs_b, values, ((1,), (0,))).astype(BF16)
    delta = jnp.sum(outs.astype(F32) * attn.astype(F32), axis=-1, keepdims=True)
    dprobs = mul(outs, values, ((1,), (1,)))
    dscores = (probs * (dprobs - delta)).astype(BF16)
    value_out[0] = mul(probs_b, outs, ((0,), (0,))).astype(BF16)
    key_out[0] = (mul(dscores, normed, ((0,), (0,))) * scale).astype(BF16)
    dnormed = mul(dscores, keys, ((1,), (0,))) * scale
    back = norm_back(raw, inverse, gain, dnormed).astype(BF16)
    for at in range(group):
        query_out[0, :, at * head_dim : (at + 1) * head_dim] = back[at * text_rows : (at + 1) * text_rows]

    @pl.when(turn == pl.num_programs(0) * heads - 1)
    def _():
        for copy in exchange(sizes, groups, vision, columns_out, *sems)[1]:
            copy.wait()


def attention(sizes, tiles, queries, out_grad, keys, values, gain, vision):
    pairs, n, heads_cut = sizes
    rows, width = vision.shape[1:]
    samples, text_rows, query_width = queries.shape
    tokens, key_width = keys.shape[1:]
    head_dim = gain.shape[1]
    heads = key_width // head_dim
    group = query_width // key_width
    wide = pl.BlockSpec((1, text_rows, group * head_dim), lambda s, h: (s, 0, h))
    tall = pl.BlockSpec((1, tokens, head_dim), lambda s, h: (s, 0, h))
    flops = samples * query_width * text_rows * tokens * 10
    part = jax.ShapeDtypeStruct((samples, tokens, key_width), BF16)
    groups = samples if heads_cut % samples == 0 else 1
    each = 1 if groups > 1 else samples
    chunks = chunks_of(width, pairs, n)
    cut = jax.ShapeDtypeStruct((chunks, pairs, each, n, rows, width // (pairs * chunks * n)), BF16)
    dma = pltpu.SemaphoreType.DMA
    return pl.pallas_call(
        functools.partial(attention_kernel, sizes, groups, group, tokens // MAX_TILES),
        grid=(samples, heads),
        out_shape=(jax.ShapeDtypeStruct(queries.shape, BF16), part, part, cut),
        in_specs=[
            pl.BlockSpec(memory_space=pltpu.SMEM),
            wide,
            wide,
            tall,
            tall,
            pl.BlockSpec((1, head_dim), lambda s, h: (0, 0)),
            pl.BlockSpec(memory_space=pltpu.HBM),
        ],
        out_specs=(wide, tall, tall, pl.BlockSpec(memory_space=pltpu.HBM)),
        scratch_shapes=[
            dma((chunks, each, pairs * n)),
            dma((chunks, each, pairs * n)),
            dma((chunks, each)),
        ],
        compiler_params=pltpu.CompilerParams(
            collective_id=5, has_side_effects=True, vmem_limit_bytes=40 * 1024 * 1024
        ),
        cost_estimate=pl.CostEstimate(flops=flops, bytes_accessed=8_000_000, transcendentals=0),
        name="attention",
    )(tiles, queries, out_grad, keys, values, gain, vision)


def local(sizes, queries, vision, key_weight, value_weight, query_gain, key_gain, out_grad, tile_count):
    pairs, n, heads_cut = sizes
    samples, rows, model_width = vision.shape
    columns = key_weight.shape[1]
    keys_all, values_all, key_raw = project(
        sizes, vision, key_weight, value_weight, key_gain[None]
    )
    query_grad, key_part, value_part, half = attention(
        sizes,
        tile_count,
        queries,
        out_grad,
        keys_all.reshape(samples, n * rows, columns),
        values_all.reshape(samples, n * rows, columns),
        query_gain[None],
        vision,
    )
    key_grad, value_grad, column_vision = ring_scatter(
        sizes,
        key_part.reshape(samples, n, rows, columns),
        value_part.reshape(samples, n, rows, columns),
        key_raw,
        key_gain[None],
        half,
        2,
    )
    every_key, every_value, vision_grad = vision_gather(
        sizes, key_grad, value_grad, key_weight, value_weight
    )
    tokens = pairs * samples * n * rows
    column_vision = column_vision.reshape(column_vision.shape[0], tokens, -1)
    outs = []
    for every in (every_key, every_value):
        grad = jnp.einsum(
            "ktd,tc->kdc", column_vision, every.reshape(tokens, columns), preferred_element_type=F32
        )
        outs.append(grad.astype(BF16))
    key_rows, value_rows = ring_gather(outs[0], outs[1], n, pairs, 4)
    return (
        query_grad,
        vision_grad.reshape(samples, rows, -1),
        key_rows.reshape(model_width, columns).astype(F32),
        value_rows.reshape(model_width, columns).astype(F32),
    )


def solution(mesh):
    sizes = (mesh.shape["dp"], mesh.shape["seq"], mesh.shape["mp"])
    in_specs = (
        P("dp", "seq", "mp"),
        P("dp", "seq", None),
        P(None, "mp"),
        P(None, "mp"),
        P(),
        P(),
        P("dp", "seq", "mp"),
        P("dp"),
    )
    out_specs = (P("dp", "seq", "mp"), P("dp", "seq", "mp"), P(None, "mp"), P(None, "mp"))
    return jax.shard_map(
        functools.partial(local, sizes), mesh=mesh, in_specs=in_specs, out_specs=out_specs, check_vma=False
    )
```
